32 devices in a mesh: layer: 8 (over z, x), rep: 4 (over y, core).
Axes of the slice: x: 2, y: 2, z: 4, core: 2. Of those that a mesh axis runs over, the one named last changes fastest.
Arguments:
- inverse_root: bfloat16 [64, 16, 128, 128], P('layer', 'rep'), may hold values from -0.625 to 0.625
- square_root: bfloat16 [64, 16, 128, 128], P('layer', 'rep'), may hold values from -0.625 to 0.625
- pattern: int32 [64, 16], P('layer', 'rep'), may hold values from 0 to 1, as said below
Outputs:
- inverse_next: bfloat16 [64, 16, 128, 128], P('layer', 'rep')
- square_next: bfloat16 [64, 16, 128, 128], P('layer', 'rep')
The draws below stay inside these ranges and needn't reach their ends.
Inputs may be any that keep to these rules, and one draw needn't show every extreme that they name: 1 marks a tile of the common pattern. Slot 8 is 1 in every block row, and slot w of block row i is 0 where i - 8 + w lies outside 0 to 63.
All inputs are finite; a program needn't handle non-finite values.
Results may differ from the reference program's by a relative error of at most 0.018.
Values may be sent and summed in bfloat16 or wider, within the bound.
A program may use at most 128 MiB of HBM per device.

```python
import jax
import jax.numpy as jnp
from jax import lax

TILE = 128
BAND = 16
HALF = 8
NB = 64
N_REP = 4


def draw_pattern(key, part):
    row_ids = jnp.arange(NB, dtype=jnp.int32)[:, None]
    slot_ids = jnp.arange(BAND, dtype=jnp.int32)[None, :]
    column = row_ids - HALF + slot_ids
    inside = (column >= 0) & (column < NB)
    key_level = jax.random.fold_in(key, 11)
    key_tiles = jax.random.fold_in(key, 23)
    fill_level = jax.random.randint(key_level, (NB, 1), 15, 90)
    tile_draws = jax.random.randint(key_tiles, (NB, BAND), 0, 100)
    chosen = (tile_draws < fill_level) | (slot_ids == HALF)
    return (inside & chosen).astype(jnp.int32)


def shard_levels(own_key, shape, shards, low, high):
    def one(position, shards_of):
        draws = jax.random.uniform(jax.random.fold_in(jax.random.fold_in(own_key, 6), position), (shards_of,), jnp.float32, low / len(shards), high / len(shards))
        return jnp.repeat(jnp.exp(draws), shape[position] // shards_of).reshape((-1,) + (1,) * (len(shape) - position - 1))

    level = one(*shards[0])
    for cut in shards[1:]:
        level = level * one(*cut)
    return level


def bell_draw(rng, shape, width, bound, pieces=(), kind=jnp.bfloat16):
    factor_of = shard_levels(rng, shape, pieces, -0.22, 0.18) if pieces else 1.0
    drawn = jax.random.normal(rng, shape, jnp.float32) * width * factor_of
    return jnp.minimum(jnp.maximum(drawn, -bound), bound).astype(kind)


def setup_inputs(seed: int = 0) -> dict:
    streams_of = jax.random.split(jax.random.key(seed), 4)
    return {
        "inverse_root": bell_draw(streams_of[0], (NB, BAND, TILE, TILE), 0.1, 0.625, ((0, 8), (1, 4))),
        "square_root": bell_draw(streams_of[1], (NB, BAND, TILE, TILE), 0.1, 0.625, ((0, 8), (1, 4))),
        "pattern": draw_pattern(jax.random.fold_in(streams_of[3], 71), 0),
    }


def band_product(left_tiles, right_tiles):
    block_rows = left_tiles.shape[0]
    band_slots = left_tiles.shape[1]
    half_band = band_slots // 2
    group_slots = band_slots // N_REP
    padded = jnp.pad(right_tiles, ((half_band, half_band), (band_slots, band_slots), (0, 0), (0, 0)))
    total = jnp.zeros(left_tiles.shape, jnp.float32)
    for group in range(N_REP):
        partial_value = jnp.zeros(left_tiles.shape, jnp.float32)
        for inner in range(group * group_slots, (group + 1) * group_slots):
            low_slot = max(0, inner - half_band)
            high_slot = min(band_slots, inner + half_band)
            offset = band_slots + half_band - inner
            shifted = padded[inner:inner + block_rows, offset + low_slot:offset + high_slot]
            product = jnp.einsum("iab,iwbc->iwac", left_tiles[:, inner].astype(jnp.float32), shifted.astype(jnp.float32))
            partial_value = partial_value.at[:, low_slot:high_slot].add(product)
        rounded = lax.optimization_barrier(partial_value.astype(jnp.bfloat16))
        total = total + rounded.astype(jnp.float32)
    return total


def reference(inverse_root, square_root, pattern):
    in_pattern = (pattern == 1)[:, :, None, None]
    inverse_kept = jnp.where(in_pattern, inverse_root, jnp.zeros_like(inverse_root))
    square_kept = jnp.where(in_pattern, square_root, jnp.zeros_like(square_root))
    intersection = jnp.where(in_pattern, band_product(inverse_kept, square_kept), jnp.float32(0.0))
    band_slots = pattern.shape[1]
    half_band = band_slots // 2
    diagonal = (jnp.arange(band_slots, dtype=jnp.int32) == half_band).astype(jnp.float32)
    identity = jnp.eye(inverse_root.shape[2], dtype=jnp.float32)
    update = jnp.where(in_pattern, 1.5 * diagonal[None, :, None, None] * identity - 0.5 * intersection, jnp.float32(0.0)).astype(jnp.bfloat16)
    square_next = jnp.where(in_pattern, band_product(square_kept, update), jnp.float32(0.0)).astype(jnp.bfloat16)
    inverse_next = jnp.where(in_pattern, band_product(update, inverse_kept), jnp.float32(0.0)).astype(jnp.bfloat16)
    return inverse_next, square_next
```

```python
import functools

import jax
import jax.numpy as jnp
from jax import lax
from jax.experimental import pallas as pl
from jax.experimental.pallas import tpu as pltpu
from jax.sharding import PartitionSpec as P

MESH = pl.DeviceIdType.MESH
ANY = pl.BlockSpec(memory_space=pl.ANY)
VMEM = pl.BlockSpec(memory_space=pltpu.VMEM)
SMEM = pl.BlockSpec(memory_space=pltpu.SMEM)


def reached(rows, band, low, high):
    half = band // 2
    found = {1: {}, -1: {}}
    for i in range(rows):
        for u in range(band):
            j = i - half + u
            if 0 <= j < rows:
                continue
            assert -rows <= j < 2 * rows
            side, a = (1, j + rows) if j < 0 else (-1, j - rows)
            for w in range(low, high):
                v = w + half - u
                if 0 <= v < band:
                    lo, hi = found[side].get(a, (v, v + 1))
                    found[side][a] = (min(lo, v), max(hi, v + 1))
    return found


def rectangles(spans, first, last):
    cut = []
    for a in sorted(spans):
        lo, hi = max(spans[a][0], first), min(spans[a][1], last)
        if lo >= hi:
            continue
        if cut and cut[-1][1] == a and cut[-1][2:] == (lo, hi):
            cut[-1] = (cut[-1][0], a + 1, lo, hi)
        else:
            cut.append((a, a + 1, lo, hi))
    return cut


def exchange_kernel(layers, reps, rows, slots, streams, *refs):
    count = len(streams)
    sources = refs[:count]
    outs = list(refs[count : len(refs) - 3])
    send_sems, recv_sems, local_sems = refs[-3:]
    band = slots * reps
    layer = lax.axis_index("layer")
    rep = lax.axis_index("rep")
    bits = []
    bit = reps // 2
    while bit >= 2:
        bits.append(bit)
        bit //= 2
    masks = list(range(0, reps, 2))
    keys = {}

    barrier = pltpu.get_barrier_semaphore()
    after, before = lax.rem(layer + 1, layers), lax.rem(layer + layers - 1, layers)
    for place in (after, before):
        pl.semaphore_signal(barrier, inc=1, device_id={"layer": place}, device_id_type=MESH)
    for flip in [1] + bits:
        partner = rep + flip * (1 - 2 * lax.rem(lax.div(rep, flip), 2))
        pl.semaphore_signal(barrier, inc=1, device_id={"rep": partner}, device_id_type=MESH)
    pl.semaphore_wait(barrier, 3 + len(bits))

    def number(key):
        return keys.setdefault(key, len(keys))

    def schedule(me):
        chip = me // 2
        spans = reached(rows, band, chip * 2 * slots, (chip + 1) * 2 * slots)
        remote = []

        def own(s):
            gather, halo = streams[s]
            if not gather:
                return sources[s]
            return outs[s].at[pl.ds(rows, rows)] if halo else outs[s]

        def shard(ref, q):
            return ref.at[:, pl.ds(q * slots, slots)]

        def copy(key, src, dst, device):
            n = number(key)
            return pltpu.make_async_remote_copy(
                src_ref=src, dst_ref=dst, send_sem=send_sems.at[n], recv_sem=recv_sems.at[n],
                device_id=device, device_id_type=MESH,
            )

        def begin(guard, made):
            remote.append((guard, made))
            if guard is None:
                made.start()
            else:
                @pl.when(guard)
                def _():
                    made.start()

        def across(s, m, bit):
            q = me ^ bit ^ m
            src = sources[s] if q == me else shard(own(s), q)
            return copy(("y", s, m), src, shard(own(s), q), {"rep": me ^ bit})

        def to_core(s, m):
            q = me ^ m
            src = sources[s] if m == 0 else shard(own(s), q)
            return copy(("d", s, m), src, shard(own(s), q), {"rep": me ^ 1})

        def halo_base(side):
            return 0 if side == 1 else 2 * rows

        def to_layer(s, side, m, k, piece):
            q = me ^ m
            a, b, lo, hi = piece
            if m == 0 and streams[s][0]:
                src = sources[s].at[pl.ds(a, b - a), pl.ds(lo - q * slots, hi - lo)]
            else:
                src = own(s).at[pl.ds(a, b - a), pl.ds(lo, hi - lo)]
            dst = outs[s].at[pl.ds(halo_base(side) + a, b - a), pl.ds(lo, hi - lo)]
            return copy(("x", s, side, m, k), src, dst, {"layer": after if side == 1 else before})

        def halo_to_core(s, side, m, q):
            cut = rectangles(spans[side], q * slots, (q + 1) * slots)
            a, b = min(c[0] for c in cut), max(c[1] for c in cut)
            part = outs[s].at[pl.ds(halo_base(side) + a, b - a), pl.ds(q * slots, slots)]
            return copy(("h", s, side, m), part, part, {"rep": me ^ 1})

        may_send = {1: layer + 1 < layers, -1: layer > 0}
        may_take = {1: layer > 0, -1: layer + 1 < layers}

        def pieces(side, m):
            q = me ^ m
            return rectangles(spans[side], q * slots, (q + 1) * slots)

        def send_layer(s, m):
            for side in (1, -1):
                for k, piece in enumerate(pieces(side, m)):
                    begin(may_send[side], to_layer(s, side, m, k, piece))

        gathered = [s for s in range(count) if streams[s][0]]
        haloed = [s for s in range(count) if streams[s][1]]
        locals_ = []
        for s in gathered:
            if bits:
                begin(None, across(s, bits[0], bits[0]))
            begin(None, to_core(s, 0))
            kept = pltpu.make_async_copy(sources[s], shard(own(s), me), local_sems.at[s])
            kept.start()
            locals_.append(kept)
        for s in haloed:
            send_layer(s, 0)
        for s in haloed:
            if not streams[s][0]:
                for m in masks[1:]:
                    send_layer(s, m)
        for s in gathered:
            held = [0]
            for n, bit in enumerate(bits):
                if n > 0:
                    for m in held:
                        begin(None, across(s, m ^ bit, bit))
                fresh = [m ^ bit for m in held]
                for m in fresh:
                    across(s, m, bit).wait_recv()
                    begin(None, to_core(s, m))
                    if streams[s][1]:
                        send_layer(s, m)
                held = held + fresh
        for m in masks:
            for s in haloed:
                for side in (1, -1):
                    cut = pieces(side, m)
                    if not cut:
                        continue
                    onward = halo_to_core(s, side, m, me ^ m)
                    remote.append((may_take[side], onward))

                    @pl.when(may_take[side])
                    def _(s=s, side=side, m=m, cut=cut, onward=onward):
                        for k, piece in enumerate(cut):
                            to_layer(s, side, m, k, piece).wait_recv()
                        onward.start()
        for s in gathered:
            for m in masks:
                copy(("d", s, m), sources[s], shard(own(s), me ^ 1 ^ m), {"rep": me ^ 1}).wait_recv()
        for s in haloed:
            for side in (1, -1):
                for m in masks:
                    if not rectangles(spans[side], (me ^ 1 ^ m) * slots, ((me ^ 1 ^ m) + 1) * slots):
                        continue

                    @pl.when(may_take[side])
                    def _(s=s, side=side, m=m):
                        halo_to_core(s, side, m, me ^ 1 ^ m).wait_recv()
        for kept in locals_:
            kept.wait()
        for guard, made in remote:
            if guard is None:
                made.wait_send()
            else:
                @pl.when(guard)
                def _(made=made):
                    made.wait_send()

    for me in range(reps):
        pl.when(rep == me)(functools.partial(schedule, me))
    assert len(keys) <= send_sems.shape[0]


def exchange(layers, reps, rows, slots, streams, arrays, call_id):
    tile = arrays[0].shape[2:]
    band = slots * reps
    shapes = [
        jax.ShapeDtypeStruct(((3 * rows if halo else rows), band) + tile, jnp.bfloat16) for _, halo in streams
    ]
    sems = 128
    return pl.pallas_call(
        functools.partial(exchange_kernel, layers, reps, rows, slots, streams),
        out_shape=shapes,
        in_specs=[VMEM if gather else ANY for gather, _ in streams],
        out_specs=[ANY] * len(streams),
        scratch_shapes=[
            pltpu.SemaphoreType.DMA((sems,)),
            pltpu.SemaphoreType.DMA((sems,)),
            pltpu.SemaphoreType.DMA((len(streams),)),
        ],
        compiler_params=pltpu.CompilerParams(collective_id=call_id, has_side_effects=True),
        name=f"exchange{call_id}",
    )(*arrays)


def product_row(i, left, right, layer, rep, layers, rows, slots, band):
    half = band // 2
    step = 4
    total = None
    for first in range(0, band, step):
        wide = jnp.concatenate([left(i, u) for u in range(first, first + step)], axis=1)
        tall = []
        for u in range(first, first + step):
            row = layer * rows + i - half + u
            inside = jnp.logical_and(row >= 0, row < layers * rows)
            tiles = []
            for w in range(slots):
                v = rep * slots + w + half - u
                good = jnp.logical_and(inside, jnp.logical_and(v >= 0, v < band))
                part = right[i + u + rows - half, jnp.clip(v, 0, band - 1)]
                tiles.append(jnp.where(good, part, jnp.zeros_like(part)))
            tall.append(jnp.concatenate(tiles, axis=1))
        piece = jnp.dot(wide, jnp.concatenate(tall, axis=0), preferred_element_type=jnp.float32)
        total = piece if total is None else total + piece
    return total


def update_kernel(layers, pattern, z_full, y_wide, out):
    rows, slots, tile = out.shape[0], out.shape[1], out.shape[2]
    band = z_full.shape[1]
    layer, rep = lax.axis_index("layer"), lax.axis_index("rep")
    across = lax.broadcasted_iota(jnp.int32, (tile, tile), 0)
    down = lax.broadcasted_iota(jnp.int32, (tile, tile), 1)
    identity = jnp.where(across == down, 1.5, 0.0).astype(jnp.float32)

    def step(i, _):
        total = product_row(i, lambda i, u: z_full[i, u], y_wide, layer, rep, layers, rows, slots, band)
        for w in range(slots):
            value = -0.5 * total[:, w * tile : (w + 1) * tile]
            value = value + jnp.where(rep * slots + w == band // 2, identity, 0.0)
            out[i, w] = jnp.where(pattern[i, w] == 1, value, 0.0).astype(out.dtype)
        return 0

    lax.fori_loop(0, rows, step, 0)


def final_kernel(layers, pattern, y_wide, u_wide, z_full, z_halo, z_next, y_next, y_own, u_all, z_all, sems):
    rows, slots, tile = z_next.shape[0], z_next.shape[1], z_next.shape[2]
    band = z_full.shape[1]
    layer, rep = lax.axis_index("layer"), lax.axis_index("rep")
    low, mid, high = pl.ds(0, rows), pl.ds(rows, rows), pl.ds(2 * rows, rows)
    copies = [
        pltpu.make_async_copy(y_wide.at[mid], y_own, sems.at[0]),
        pltpu.make_async_copy(u_wide, u_all, sems.at[1]),
        pltpu.make_async_copy(z_halo.at[low], z_all.at[low], sems.at[2]),
        pltpu.make_async_copy(z_full, z_all.at[mid], sems.at[3]),
        pltpu.make_async_copy(z_halo.at[high], z_all.at[high], sems.at[4]),
    ]
    for made in copies:
        made.start()
    for made in copies:
        made.wait()

    def step(i, _):
        jobs = (
            (lambda i, u: y_own[i, u], u_all, y_next),
            (lambda i, u: u_all[i + rows, u], z_all, z_next),
        )
        for left, right, out in jobs:
            total = product_row(i, left, right, layer, rep, layers, rows, slots, band)
            for w in range(slots):
                value = total[:, w * tile : (w + 1) * tile]
                out[i, w] = jnp.where(pattern[i, w] == 1, value, 0.0).astype(out.dtype)
        return 0

    lax.fori_loop(0, rows, step, 0)


def solution(mesh):
    layers, reps = mesh.shape["layer"], mesh.shape["rep"]

    def body(inverse_root, square_root, pattern):
        rows, slots = pattern.shape
        tile = inverse_root.shape[2:]
        band = slots * reps
        in_pattern = (pattern == 1)[:, :, None, None]
        z = jnp.where(in_pattern, inverse_root, jnp.zeros_like(inverse_root))
        y = jnp.where(in_pattern, square_root, jnp.zeros_like(square_root))
        limit = pltpu.CompilerParams(vmem_limit_bytes=56 * 1024 * 1024)
        local = jax.ShapeDtypeStruct((rows, slots) + tile, jnp.bfloat16)
        y_wide, z_full = exchange(layers, reps, rows, slots, ((True, True), (True, False)), (y, z), 0)
        u = pl.pallas_call(
            functools.partial(update_kernel, layers),
            out_shape=local,
            in_specs=[SMEM, VMEM, VMEM],
            out_specs=VMEM,
            compiler_params=limit,
            name="update",
        )(pattern, z_full, y_wide)
        u_wide, z_halo = exchange(layers, reps, rows, slots, ((True, True), (False, True)), (u, z_full), 1)
        z_next, y_next = pl.pallas_call(
            functools.partial(final_kernel, layers),
            out_shape=[local, local],
            in_specs=[SMEM, ANY, ANY, ANY, ANY],
            out_specs=[VMEM, VMEM],
            scratch_shapes=[
                pltpu.VMEM((rows, band) + tile, jnp.bfloat16),
                pltpu.VMEM((3 * rows, band) + tile, jnp.bfloat16),
                pltpu.VMEM((3 * rows, band) + tile, jnp.bfloat16),
                pltpu.SemaphoreType.DMA((5,)),
            ],
            compiler_params=limit,
            name="final",
        )(pattern, y_wide, u_wide, z_full, z_halo)
        return z_next, y_next

    placed = P("layer", "rep", None, None)
    return jax.shard_map(
        body,
        mesh=mesh,
        in_specs=(placed, placed, P("layer", "rep")),
        out_specs=(placed, placed),
        check_vma=False,
    )
```

```python
import functools

import jax
import jax.numpy as jnp
from jax import lax
from jax.experimental import pallas as pl
from jax.experimental.pallas import tpu as pltpu
from jax.sharding import PartitionSpec as P

MESH = pl.DeviceIdType.MESH
VMEM = pl.BlockSpec(memory_space=pltpu.VMEM)
SMEM = pl.BlockSpec(memory_space=pltpu.SMEM)
SEMAPHORES = 256


def reached(rows, band, low, high):
    half = band // 2
    found = {1: {}, -1: {}}
    for i in range(rows):
        for u in range(band):
            j = i - half + u
            if 0 <= j < rows:
                continue
            assert -rows <= j < 2 * rows
            side, a = (1, j + rows) if j < 0 else (-1, j - rows)
            for w in range(low, high):
                v = w + half - u
                if 0 <= v < band:
                    lo, hi = found[side].get(a, (v, v + 1))
                    found[side][a] = (min(lo, v), max(hi, v + 1))
    return found


def rectangles(spans, first, last):
    cut = []
    for a in sorted(spans):
        lo, hi = max(spans[a][0], first), min(spans[a][1], last)
        if lo >= hi:
            continue
        if cut and cut[-1][1] == a and cut[-1][2:] == (lo, hi):
            cut[-1] = (cut[-1][0], a + 1, lo, hi)
        else:
            cut.append((a, a + 1, lo, hi))
    return cut


class Later:
    def __init__(self, make, args=None):
        self.make, self.args = make, args

    def __call__(self, *args):
        return Later(self.make, args)

    def start(self):
        self.make(*self.args).start()

    def wait_recv(self):
        self.make(*self.args).wait_recv()

    def wait_send(self):
        self.make(*self.args).wait_send()


def step_kernel(layers, reps, refs_shape, pattern, z_own, y_own, z_next, y_next, y_wide, z_wide, u_wide, send_sems, recv_sems):
    rows, slots, tile = refs_shape
    band = slots * reps
    half = band // 2
    layer, rep = lax.axis_index("layer"), lax.axis_index("rep")
    after, before = lax.rem(layer + 1, layers), lax.rem(layer + layers - 1, layers)
    may_send = {1: layer + 1 < layers, -1: layer > 0}
    may_take = {1: layer > 0, -1: layer + 1 < layers}
    bits = []
    bit = reps // 2
    while bit >= 2:
        bits.append(bit)
        bit //= 2
    masks = list(range(0, reps, 2))
    keys = {}
    wides = {"y": y_wide, "z": z_wide, "u": u_wide}
    relayed = ("z", "u") if reps == 4 else ()

    def keep(i, _):
        for w in range(slots):
            good = pattern[i, w] == 1
            for own, wide in ((y_own, y_wide), (z_own, z_wide)):
                part = own[i, w]
                wide[rows + i, rep * slots + w] = jnp.where(good, part, jnp.zeros_like(part))
        return 0

    lax.fori_loop(0, rows, keep, 0)

    barrier = pltpu.get_barrier_semaphore()
    for place in (after, before):
        pl.semaphore_signal(barrier, inc=1, device_id={"layer": place}, device_id_type=MESH)
    for flip in [1] + bits:
        partner = rep + flip * (1 - 2 * lax.rem(lax.div(rep, flip), 2))
        pl.semaphore_signal(barrier, inc=1, device_id={"rep": partner}, device_id_type=MESH)
    pl.semaphore_wait(barrier, 3 + len(bits))

    def schedule(me):
        chip = me // 2
        remote = []
        need = reached(rows, band, chip * 2 * slots, (chip + 1) * 2 * slots)
        union = reached(rows, band, 0, band)
        other = reached(rows, band, (1 - chip) * 2 * slots, (2 - chip) * 2 * slots) if relayed else None
        direct_side = 1 if chip == 0 else -1

        def spans(s, side):
            if s not in relayed:
                return need[side]
            return union[side] if side == direct_side else {}

        def arriving(s, side):
            return spans(s, side) or need[side]

        def cut(which, q):
            return rectangles(which, q * slots, (q + 1) * slots)

        def base(side):
            return 0 if side == 1 else 2 * rows

        def copy(key, src, dst, device):
            n = keys.setdefault(key, len(keys))
            return pltpu.make_async_remote_copy(
                src_ref=src, dst_ref=dst, send_sem=send_sems.at[n], recv_sem=recv_sems.at[n],
                device_id=device, device_id_type=MESH,
            )

        def begin(guard, made):
            remote.append((guard, made))
            if guard is None:
                made.start()
            else:
                pl.when(guard)(made.start)

        def shard(s, q):
            return wides[s].at[pl.ds(rows, rows), pl.ds(q * slots, slots)]

        @Later
        def across(s, m, bit):
            part = shard(s, me ^ bit ^ m)
            return copy(("y", s, m), part, part, {"rep": me ^ bit})

        @Later
        def across_in(s, m, bit):
            part = shard(s, me ^ m)
            return copy(("y", s, m), part, part, {"rep": me ^ bit})

        @Later
        def to_core(s, m):
            part = shard(s, me ^ m)
            return copy(("d", s, m), part, part, {"rep": me ^ 1})

        @Later
        def to_core_in(s, m):
            part = shard(s, me ^ 1 ^ m)
            return copy(("d", s, m), part, part, {"rep": me ^ 1})

        @Later
        def to_layer(s, side, m, k, piece):
            a, b, lo, hi = piece
            src = wides[s].at[pl.ds(rows + a, b - a), pl.ds(lo, hi - lo)]
            dst = wides[s].at[pl.ds(base(side) + a, b - a), pl.ds(lo, hi - lo)]
            return copy(("x", s, side, m, k), src, dst, {"layer": after if side == 1 else before})

        @Later
        def relay(s, side, m, k, piece):
            a, b, lo, hi = piece
            part = wides[s].at[pl.ds(base(side) + a, b - a), pl.ds(lo, hi - lo)]
            return copy(("r", s, side, m, k), part, part, {"rep": me ^ 2})

        @Later
        def halo_to_core(s, side, m, q):
            pieces = cut(arriving(s, side), q)
            a, b = min(c[0] for c in pieces), max(c[1] for c in pieces)
            part = wides[s].at[pl.ds(base(side) + a, b - a), pl.ds(q * slots, slots)]
            return copy(("h", s, side, m), part, part, {"rep": me ^ 1})

        def send_layer(s, m):
            for side in (1, -1):
                for k, piece in enumerate(cut(spans(s, side), me ^ m)):
                    begin(may_send[side], to_layer(s, side, m, k, piece))

        def take_direct(s, m):
            for side in (1, -1):
                pieces = cut(spans(s, side), me ^ m)
                if pieces:
                    made = [to_layer(s, side, m, k, piece) for k, piece in enumerate(pieces)]
                    onward = [halo_to_core(s, side, m, me ^ m)]
                    if s in relayed:
                        onward += [
                            relay(s, side, m ^ 2, k, piece)
                            for k, piece in enumerate(cut(other[side], me ^ m))
                        ]
                    pass_on(side, made, onward)

        def take_relayed(s, m):
            for side in (1, -1):
                if s in relayed and side != direct_side:
                    pieces = cut(need[side], me ^ m)
                    if pieces:
                        made = [relay(s, side, m, k, piece) for k, piece in enumerate(pieces)]
                        pass_on(side, made, [halo_to_core(s, side, m, me ^ m)])

        def pass_on(side, made, onward):
            remote.extend((may_take[side], o) for o in onward)

            @pl.when(may_take[side])
            def _():
                for one in made:
                    one.wait_recv()
                for one in onward:
                    one.start()

        def start_gather(s):
            if bits:
                begin(None, across(s, bits[0], bits[0]))
            begin(None, to_core(s, 0))

        def gather(s, halo):
            held = [0]
            for n, bit in enumerate(bits):
                if n > 0:
                    for m in held:
                        begin(None, across(s, m ^ bit, bit))
                fresh = [m ^ bit for m in held]
                for m in fresh:
                    across_in(s, m, bit).wait_recv()
                    begin(None, to_core(s, m))
                    if halo:
                        send_layer(s, m)
                held = held + fresh

        def finish_own(s):
            for m in masks:
                to_core_in(s, m).wait_recv()

        def finish_halo(s):
            for side in (1, -1):
                made = [
                    halo_to_core(s, side, m, me ^ 1 ^ m)
                    for m in masks
                    if cut(arriving(s, side), me ^ 1 ^ m)
                ]

                @pl.when(may_take[side])
                def _():
                    for one in made:
                        one.wait_recv()

        start_gather("y")
        start_gather("z")
        send_layer("y", 0)
        gather("y", True)
        send_layer("z", 0)
        take_direct("y", 0)
        gather("z", True)
        for m in masks[1:]:
            take_direct("y", m)
        for s in ("y", "z"):
            finish_own(s)
        finish_halo("y")
        yield
        start_gather("u")
        send_layer("u", 0)
        for m in masks:
            take_direct("z", m)
        gather("u", True)
        for m in masks:
            take_relayed("z", m)
        finish_own("u")
        finish_halo("z")
        yield
        for m in masks:
            take_direct("u", m)
        for m in masks:
            take_relayed("u", m)
        finish_halo("u")
        yield
        for guard, made in remote:
            if guard is None:
                made.wait_send()
            else:
                pl.when(guard)(made.wait_send)
        yield

    plans = [schedule(me) for me in range(reps)]

    def advance():
        for me in range(reps):
            pl.when(rep == me)(functools.partial(next, plans[me]))

    down = lax.broadcasted_iota(jnp.int32, (tile, tile), 0)
    right = lax.broadcasted_iota(jnp.int32, (tile, tile), 1)
    identity = jnp.where(down == right, 1.5, 0.0).astype(jnp.float32)

    def multiply(left, right, store):
        def step(i, _):
            total = product_row(i, left, right, layer, rep, layers, rows, slots, band)
            for w in range(slots):
                store(i, w, pattern[i, w] == 1, total[:, w * tile : (w + 1) * tile])
            return 0

        lax.fori_loop(0, rows, step, 0)

    def store_update(i, w, good, value):
        value = -0.5 * value + jnp.where(rep * slots + w == half, identity, 0.0)
        u_wide[rows + i, rep * slots + w] = jnp.where(good, value, 0.0).astype(jnp.bfloat16)

    def store_inverse(i, w, good, value):
        z_next[i, w] = jnp.where(good, value, 0.0).astype(jnp.bfloat16)

    def store_square(i, w, good, value):
        y_next[i, w] = jnp.where(good, value, 0.0).astype(jnp.bfloat16)

    advance()
    multiply(z_wide, y_wide, store_update)
    advance()
    multiply(u_wide, z_wide, store_inverse)
    advance()
    multiply(y_wide, u_wide, store_square)
    advance()
    assert len(keys) <= send_sems.shape[0]


def product_row(i, left, right, layer, rep, layers, rows, slots, band):
    half = band // 2
    step = 4
    total = None
    for first in range(0, band, step):
        wide = jnp.concatenate([left[rows + i, u] for u in range(first, first + step)], axis=1)
        tall = []
        for u in range(first, first + step):
            row = layer * rows + i - half + u
            inside = jnp.logical_and(row >= 0, row < layers * rows)
            tiles = []
            for w in range(slots):
                v = rep * slots + w + half - u
                good = jnp.logical_and(inside, jnp.logical_and(v >= 0, v < band))
                part = right[i + u + rows - half, lax.rem(v + band, band)]
                tiles.append(jnp.where(good, part, jnp.zeros_like(part)))
            tall.append(jnp.concatenate(tiles, axis=1))
        piece = jnp.dot(wide, jnp.concatenate(tall, axis=0), preferred_element_type=jnp.float32)
        total = piece if total is None else total + piece
    return total


def solution(mesh):
    layers, reps = mesh.shape["layer"], mesh.shape["rep"]

    def body(inverse_root, square_root, pattern):
        rows, slots = pattern.shape
        tile = inverse_root.shape[2:]
        local = jax.ShapeDtypeStruct((rows, slots) + tile, jnp.bfloat16)
        wide = pltpu.VMEM((3 * rows, slots * reps) + tile, jnp.bfloat16)
        return pl.pallas_call(
            functools.partial(step_kernel, layers, reps, (rows, slots, tile[0])),
            out_shape=(local, local),
            in_specs=[SMEM, VMEM, VMEM],
            out_specs=(VMEM, VMEM),
            scratch_shapes=[
                wide,
                wide,
                wide,
                pltpu.SemaphoreType.DMA((SEMAPHORES,)),
                pltpu.SemaphoreType.DMA((SEMAPHORES,)),
            ],
            compiler_params=pltpu.CompilerParams(
                collective_id=0, has_side_effects=True, vmem_limit_bytes=60 * 1024 * 1024
            ),
            name="newton_step",
        )(pattern, inverse_root, square_root)

    placed = P("layer", "rep", None, None)
    return jax.shard_map(
        body,
        mesh=mesh,
        in_specs=(placed, placed, P("layer", "rep")),
        out_specs=(placed, placed),
        check_vma=False,
    )
```
